256 devices in a mesh: parts: 2 (over z), genes: 64 (over x, y), samples: 2 (over core).
Axes of the slice: x: 8, y: 8, z: 2, core: 2. Of those that a mesh axis runs over, the one named last changes fastest.
The devices are a block of a 8x8x16 slice.
Arguments:
- dosage: bfloat16 [262144, 2048], P(('parts', 'genes'), 'samples'), parts along dimension 0, may hold values from -6 to 6
- expression: bfloat16 [1024, 2048], P(('parts', 'genes'), 'samples'), parts along dimension 0, may hold values from -6 to 6
- intron_counts: bfloat16 [4096, 20480], P(('parts', 'samples', 'genes')), parts along dimension 0, may hold values from 1 to 100
- cluster_sizes: int32 [1024, 8], P('parts'), parts along dimension 0, may hold values from 1 to 12, 40 in all within a row
- valid_mask: int32 [1024, 40], P('parts'), parts along dimension 0, may hold values 0 or 1
- gene_block: int32 [1024], P('parts'), parts along dimension 0, may hold values from 0 to 511, each once
- window_start: int32 [1024], P(('parts', 'genes')), parts along dimension 0, may hold values from 0 to 1024, as said below
Outputs:
- assoc: bfloat16 [1024, 41, 2048], P(('parts', 'genes'), None, 'samples'), parts along dimension 0
The draws below stay inside these ranges and needn't reach their ends.
There are 2 independent parts, one for each index of `parts`. The reference program is written for one: setup_inputs(seed, part) draws one part's arguments, and reference() takes and returns one part's arrays. A program takes and returns all parts, laid end to end along the dimension named above; each array names one. Nothing has to cross between parts.
Inputs may be any that keep to these rules, and one draw needn't show every extreme that they name: Every window_start is a multiple of 128 and at most 1024; some gene reaches 1024 in every draw. `gene_block`: a permutation of the genes. `cluster_sizes`: each row sums to 40.
All inputs are finite; a program needn't handle non-finite values.
Results may differ from the reference program's by a relative error of at most 0.0058.
Values may be sent and summed in bfloat16 or wider, within the bound.
No kernel may reach another device: no remote copies, remote signals or barrier semaphores. Data moves between devices by JAX's collectives and lax.ppermute only.
A program may use at most 64 MiB of HBM per device.

```python
import math
import jax
import jax.numpy as jnp
import numpy as np
from jax import lax

GENE_DEV = 8
W = 2048
SLOTS = 40
CLUST = 8
CL_MOST = 12
SPILL = 1024
ALIGN = 128
PHEN = 41
GENES = 512
SAMP = 2048
VARIANTS = 131072
INTRONS = 20480
N_GENES = 64


def draw_window_start(key, part):
    draw_starts, draw_pick = jax.random.split(jax.random.fold_in(key, 7))
    starts = jax.random.randint(draw_starts, (GENES,), 0, SPILL // ALIGN + 1, dtype=jnp.int32) * ALIGN
    chosen = jax.random.randint(draw_pick, (), 0, GENES, dtype=jnp.int32)
    return jnp.where(jnp.arange(GENES, dtype=jnp.int32) == chosen, SPILL, starts).astype(jnp.int32)


def plant(array, key, least, high):
    spot = [jax.random.randint(jax.random.fold_in(key, axis), (), 0, length) for axis, length in enumerate(array.shape)]
    main_axis = array.shape.index(max(array.shape))
    neighbour = spot[:main_axis] + [(spot[main_axis] + 1) % array.shape[main_axis]] + spot[main_axis + 1:]
    return array.at[tuple(spot)].set(least).at[tuple(neighbour)].set(high)


def steps_of(own_key, shape, cuts, least, high):
    def one(dim, parts):
        heights = jax.random.uniform(jax.random.fold_in(jax.random.fold_in(own_key, 6), dim), (parts,), jnp.float32, least / len(cuts), high / len(cuts))
        return jnp.repeat(jnp.exp(heights), shape[dim] // parts).reshape((-1,) + (1,) * (len(shape) - dim - 1))

    factor_of = one(*cuts[0])
    for cut in cuts[1:]:
        factor_of = factor_of * one(*cut)
    return factor_of


def split_up(amount, total, most, lean):
    loads = [(1 << 20) // math.isqrt(rank ** lean) + 1 for rank in range(2, amount + 1)]
    spare, given = total - most - (amount - 1), [1] * (amount - 1)
    while spare > 0:
        movable = [i for i in range(amount - 1) if given[i] < most]
        mass, left = sum([loads[i] for i in movable]), spare
        for i in movable:
            more = min(most - given[i], max(1, left * loads[i] // mass), spare)
            given[i] = given[i] + more
            spare = spare - more
    return np.array([most] + given)


def uneven(key, count, total, bound, slope):
    if count == 2:
        one = jax.random.randint(key, (), max(1, total - bound), min(bound, total - 1) + 1)
        return jnp.stack([one, total - one])
    sizes = jnp.asarray(split_up(count, total, bound, slope), jnp.int32)
    couples = (count - 1) // 2
    giver, taker = sizes[1:1 + 2 * couples:2], sizes[2:2 + 2 * couples:2]
    slack = jnp.minimum(giver - 1, bound - taker)
    passed = jax.random.randint(jax.random.fold_in(key, 1), (couples,), 0, 1 << 20) % (slack + 1)
    sizes = sizes.at[1:1 + 2 * couples:2].set(giver - passed).at[2:2 + 2 * couples:2].set(taker + passed)
    return sizes[jax.random.permutation(jax.random.fold_in(key, 2), count)]


def scatter_about(own_key, shape, scale, bound, shards=(), held_as=jnp.bfloat16):
    entries = scale * jax.random.normal(own_key, shape, jnp.float32)
    if shards:
        entries = entries * steps_of(own_key, shape, shards, -0.22, 0.18)
    return jnp.clip(entries, -bound, bound).astype(held_as)


def setup_inputs(seed: int = 0, part: int = 0) -> dict:
    splits = jax.random.split(jax.random.key(seed), 8)
    own_keys = jax.random.split(jax.random.fold_in(splits[7], part), 8)
    dosage = scatter_about(own_keys[0], (VARIANTS, SAMP), 1.0, 6.0, ((0, 64), (1, 2)))
    expression = scatter_about(own_keys[1], (GENES, SAMP), 1.0, 6.0, ((0, 64), (1, 2)))
    intron_counts = jnp.clip(jnp.exp(math.log(100.0) - 4.6051702 * jax.random.uniform(own_keys[2], (SAMP, INTRONS), jnp.float32) ** steps_of(own_keys[2], (SAMP, INTRONS), ((0, 128),), -0.2, 0.2)), 1.0, 100.0).astype(jnp.bfloat16)
    cluster_sizes = jax.vmap(lambda own: uneven(own, CLUST, SLOTS, CL_MOST, 2))(jax.random.split(own_keys[3], GENES)).reshape((GENES, CLUST)).astype(jnp.int32)
    valid_mask = plant((jax.random.randint(own_keys[4], (GENES, SLOTS), 0, 4) < 3).astype(jnp.int32), jax.random.fold_in(own_keys[4], 1), 0, 1)
    gene_block = jax.random.permutation(own_keys[5], GENES).astype(jnp.int32)
    window_start = draw_window_start(jax.random.fold_in(jax.random.fold_in(splits[7], part), 71), part)
    return dict(dosage=dosage, expression=expression, intron_counts=intron_counts, cluster_sizes=cluster_sizes, valid_mask=valid_mask, gene_block=gene_block, window_start=window_start)


def cluster_ratios(counts, cluster_sizes, valid_mask):
    cluster_ends = jnp.cumsum(cluster_sizes, axis=1, dtype=jnp.int32)
    slot_index = jnp.arange(SLOTS, dtype=jnp.int32)
    cluster_id = lax.optimization_barrier(jnp.sum((cluster_ends[:, None, :] <= slot_index[None, :, None]).astype(jnp.int32), axis=2, dtype=jnp.int32))
    same_cluster = (cluster_id[:, :, None] == cluster_id[:, None, :]).astype(jnp.float32)
    live_counts = counts * valid_mask.astype(jnp.float32)[None, :, :]
    cluster_total = jnp.einsum('sgj,gjk->sgk', live_counts, same_cluster, precision=lax.Precision.HIGHEST)
    return (live_counts / jnp.maximum(cluster_total, 1.0)).astype(jnp.bfloat16)

def tile_window(owner_block, offset, width):
    leading = owner_block.shape[:-1]
    tiles = owner_block.reshape(leading + (owner_block.shape[-1] // ALIGN, ALIGN))
    first_tile = (offset // ALIGN).astype(jnp.int32)
    piece = lax.dynamic_slice_in_dim(tiles, first_tile, width // ALIGN, len(leading))
    return piece.reshape(leading + (width,))

def window_slices(product, row_sum, row_square, starts):

    def window_of(owner_block, offset):
        return tile_window(owner_block, offset, W)
    cross_part = jax.vmap(window_of, in_axes=(0, 0))(product, starts)
    sum_part = jax.vmap(window_of, in_axes=(None, 0))(row_sum, starts)
    square_part = jax.vmap(window_of, in_axes=(None, 0))(row_square, starts)
    return (cross_part, sum_part, square_part)

def finish_stats(cross_part, sum_part, square_part, phen_sum, phen_square, sample_count):
    numerator = cross_part - sum_part[:, None, :] * phen_sum[:, :, None] / sample_count
    dose_var = jnp.maximum(square_part - sum_part * sum_part / sample_count, 1.0)
    pheno_var = jnp.maximum(phen_square - phen_sum * phen_sum / sample_count, 1.0)
    return (numerator * lax.rsqrt(dose_var)[:, None, :] * lax.rsqrt(pheno_var)[:, :, None]).astype(jnp.bfloat16)

def reference(dosage, expression, intron_counts, cluster_sizes, valid_mask, gene_block, window_start):
    padded = jnp.concatenate([dosage, jnp.zeros((SPILL, SAMP), jnp.bfloat16)], axis=0)
    stored = intron_counts.reshape(SAMP, GENES, SLOTS)

    def owner_stats(owner_index):
        gene_ids = owner_index * GENE_DEV + jnp.arange(GENE_DEV, dtype=jnp.int32)
        dose_rows = lax.dynamic_slice_in_dim(padded, owner_index * W, W + SPILL, 0)
        counts = jnp.take(stored, gene_block[gene_ids], axis=1).astype(jnp.float32)
        ratios = cluster_ratios(counts, cluster_sizes[gene_ids], valid_mask[gene_ids])
        expr_rows = lax.dynamic_slice_in_dim(expression, owner_index * GENE_DEV, GENE_DEV, 0)
        pheno_panel = jnp.concatenate([expr_rows.T[:, :, None], ratios], axis=2).reshape(SAMP, GENE_DEV * PHEN)
        product = lax.dot_general(pheno_panel, dose_rows, (((0,), (1,)), ((), ())), preferred_element_type=jnp.float32)
        product = product.reshape(GENE_DEV, PHEN, W + SPILL)
        dose_float = dose_rows.astype(jnp.float32)
        row_sum = lax.optimization_barrier(jnp.sum(dose_float, axis=1))
        row_square = lax.optimization_barrier(jnp.sum(dose_float * dose_float, axis=1))
        pheno_float = pheno_panel.astype(jnp.float32)
        phen_sum = lax.optimization_barrier(jnp.sum(pheno_float, axis=0)).reshape(GENE_DEV, PHEN)
        phen_square = lax.optimization_barrier(jnp.sum(pheno_float * pheno_float, axis=0)).reshape(GENE_DEV, PHEN)
        cross_part, sum_part, square_part = window_slices(product, row_sum, row_square, window_start[gene_ids])
        return finish_stats(cross_part, sum_part, square_part, phen_sum, phen_square, float(SAMP))
    result = lax.map(owner_stats, jnp.arange(N_GENES, dtype=jnp.int32))
    return result.reshape(GENES, PHEN, W)
```

```python
import functools

import jax
import jax.numpy as jnp
from jax import lax
from jax.experimental import pallas as pl
from jax.experimental.pallas import tpu as pltpu
from jax.sharding import PartitionSpec as P


W = 2048
SLOTS = 40
CLUST = 8
SPILL = 1024
HALF = 1024
GENE_DEV = 8
GROUP = 4
LANES = 128
WIDE = 384
RATIOS = SLOTS * GROUP
ROWS = RATIOS + 8
ONES = RATIOS + GROUP
F32 = jnp.float32
BF16 = jnp.bfloat16

VMEM = pl.BlockSpec(memory_space=pltpu.VMEM)
SMEM = pl.BlockSpec(memory_space=pltpu.SMEM)
HBM = pl.BlockSpec(memory_space=pltpu.HBM)


def params(mib):
    return pltpu.CompilerParams(vmem_limit_bytes=mib * 1024 * 1024)


def cost(flops, nbytes):
    return pl.CostEstimate(flops=flops, bytes_accessed=nbytes, transcendentals=0)


def gather_kernel(block_hbm, counts_hbm, out_ref, block_ref, counts_ref, sems):
    blocks_in = pltpu.make_async_copy(block_hbm, block_ref, sems.at[0])
    counts_in = pltpu.make_async_copy(counts_hbm, counts_ref, sems.at[1])
    blocks_in.start()
    counts_in.start()
    samples = counts_ref.shape[0]
    owners = out_ref.shape[0]
    last = counts_ref.shape[1] // LANES - 1
    lane = lax.broadcasted_iota(jnp.int32, (samples, LANES), 1)
    low = lax.broadcasted_iota(jnp.int32, (samples // 2, LANES), 1) < 64
    out_ref[0, 0:40, :] = jnp.zeros((40, LANES), BF16)
    blocks_in.wait()
    counts_in.wait()

    def column(index):
        start = pl.multiple_of(index * LANES, LANES)
        return counts_ref[:, pl.ds(start, LANES)].astype(F32)

    def owner(o, carry):
        g = []
        for i in range(GENE_DEV):
            first = block_ref[o * GENE_DEV + i] * SLOTS
            tile = lax.shift_right_logical(first, 7)
            inside = first & (LANES - 1)
            both = jnp.where(
                lane >= inside, column(tile), column(jnp.minimum(tile + 1, last))
            )
            g.append(pltpu.roll(both, (SLOTS * i - inside) & (LANES - 1), 1))
        a = jnp.where(lane < 40, g[0], jnp.where(lane < 80, g[1], jnp.where(lane < 120, g[2], g[3])))
        b = jnp.where(lane < 32, g[3], jnp.where(lane < 72, g[4], jnp.where(lane < 112, g[5], g[6])))
        c = jnp.where(lane < 24, g[6], g[7])
        packed = jnp.where(low, c[: samples // 2], pltpu.roll(c[samples // 2 :], 64, 1))
        after = jnp.minimum(o + 1, owners - 1)
        for at, row in ((after, 0), (o, 40)):
            out_ref[at, row : row + 16, :] = a.astype(BF16)
            out_ref[at, row + 16 : row + 32, :] = b.astype(BF16)
            out_ref[at, row + 32 : row + 40, :] = packed.astype(BF16)
        return carry

    owner(owners - 1, 0)
    lax.fori_loop(0, owners - 1, owner, 0, unroll=9)


def gather_blocks(gene_block, counts, owners):
    return pl.pallas_call(
        gather_kernel,
        out_shape=jax.ShapeDtypeStruct((owners, 80, LANES), BF16),
        in_specs=[HBM, HBM],
        out_specs=VMEM,
        scratch_shapes=[
            pltpu.SMEM(gene_block.shape, jnp.int32),
            pltpu.VMEM(counts.shape, BF16),
            pltpu.SemaphoreType.DMA((2,)),
        ],
        compiler_params=params(8),
        cost_estimate=cost(10_000_000, 1),
        name="gather_blocks",
    )(gene_block, counts)


def panel_kernel(behind, recv_ref, expr_ref, sizes_ref, valid_ref, keep_ref, give_ref):
    me = jnp.maximum(lax.axis_index("genes") - behind, 0)
    first_core = lax.axis_index("samples") == 0
    first = me * GENE_DEV
    start = pl.multiple_of(first // LANES * LANES, LANES)
    back = (LANES - first % LANES) & (LANES - 1)
    sizes = pltpu.roll(sizes_ref[:, pl.ds(start, LANES)].astype(F32), back, 1)
    valid = pltpu.roll(valid_ref[:, pl.ds(start, LANES)].astype(F32), back, 1)
    ends, running = [], jnp.zeros((1, LANES), F32)
    for c in range(CLUST):
        running = running + sizes[c : c + 1, :]
        ends.append(running)
    ends = jnp.concatenate(ends, axis=0)

    x = lax.broadcasted_iota(jnp.int32, (LANES, WIDE), 1)
    i = lax.broadcasted_iota(jnp.int32, (LANES, WIDE), 0)
    spread = jnp.where((x >= SLOTS * i) & (x < SLOTS * i + SLOTS) & (i < GENE_DEV), 1.0, 0.0)
    spread = spread.astype(BF16)

    def slots_of(rows):
        x = lax.broadcasted_iota(jnp.int32, (rows, WIDE), 1)
        base = jnp.zeros((rows, WIDE), jnp.int32)
        for gene in range(1, GENE_DEV + 1):
            base = jnp.where(x >= SLOTS * gene, SLOTS * gene, base)
        return base, x - base

    ends_at = jnp.dot(ends.astype(BF16), spread, preferred_element_type=F32)
    base, slot = slots_of(CLUST)
    slot = slot.astype(F32)
    low = jnp.max(jnp.where(ends_at <= slot, ends_at, 0.0), axis=0, keepdims=True)
    high = jnp.min(jnp.where(ends_at > slot, ends_at, float(SLOTS)), axis=0, keepdims=True)
    base = base[0:1, :].astype(F32)
    valid_at = jnp.dot(valid.astype(BF16), spread, preferred_element_type=F32)
    _, slot40 = slots_of(SLOTS)
    row40 = lax.broadcasted_iota(jnp.int32, (SLOTS, WIDE), 0)
    live = jnp.sum(jnp.where(slot40 == row40, valid_at, 0.0), axis=0, keepdims=True)

    k = lax.broadcasted_iota(jnp.int32, (WIDE, WIDE), 0).astype(F32)
    inside = (k >= base + low) & (k < base + high)
    same = jnp.where(inside & (k < float(SLOTS * GENE_DEV)), 1.0, 0.0).astype(BF16)

    per = LANES // 16
    for t in range(recv_ref.shape[0] // per):
        owned = 40 * (1 - behind)
        piece = recv_ref[t * per : (t + 1) * per, owned : owned + 40, :].astype(F32)
        a = piece[:, 0:16, :].reshape(LANES, LANES)
        b = piece[:, 16:32, :].reshape(LANES, LANES)
        c = piece[:, 32:40, :]
        swapped = pltpu.roll(c, 64, 2)
        c = jnp.concatenate([c, swapped], axis=1).reshape(LANES, LANES)
        counts = jnp.concatenate([a, b, c], axis=1) * live
        total = jnp.dot(counts.astype(BF16), same, preferred_element_type=F32)
        ratio = counts / jnp.maximum(total, 1.0)
        lanes = slice(t * LANES, (t + 1) * LANES)
        turned = jnp.transpose(ratio)
        low_half, high_half = turned[0:RATIOS], turned[RATIOS : 2 * RATIOS]
        keep_ref[0:RATIOS, lanes] = jnp.where(first_core, low_half, high_half).astype(BF16)
        give_ref[0:RATIOS, lanes] = jnp.where(first_core, high_half, low_half).astype(BF16)
    expr = expr_ref[...].astype(F32)
    row = lax.broadcasted_iota(jnp.int32, expr.shape, 0)
    low_half = jnp.where(row < GROUP, expr, 1.0)
    high_half = jnp.where(row < GROUP, pltpu.roll(expr, GROUP, 0), 1.0)
    keep_ref[RATIOS:ROWS, :] = jnp.where(first_core, low_half, high_half).astype(BF16)
    give_ref[RATIOS:ROWS, :] = jnp.where(first_core, high_half, low_half).astype(BF16)


def make_panel(recv, expression, sizes, valid, behind):
    half = jax.ShapeDtypeStruct((ROWS, expression.shape[1]), BF16)
    return pl.pallas_call(
        functools.partial(panel_kernel, behind),
        out_shape=(half, half),
        in_specs=[VMEM] * 4,
        out_specs=(VMEM, VMEM),
        compiler_params=params(16),
        cost_estimate=cost(400_000_000, 1_400_000),
        name="make_panel",
    )(recv, expression, sizes, valid)


NT = (((1,), (1,)), ((), ()))


def row_sums(panels):
    rows = panels[0].shape[0]
    one, two = jnp.zeros((rows, LANES), F32), jnp.zeros((rows, LANES), F32)
    for panel in panels:
        for t in range(panel.shape[1] // LANES):
            p = panel[:, t * LANES : (t + 1) * LANES].astype(F32)
            one, two = one + p, two + p * p
    return jnp.sum(one, axis=1, keepdims=True), jnp.sum(two, axis=1, keepdims=True)


def square_sums(doses):
    block = doses[0].shape[0]
    folded = jnp.zeros((block, LANES), F32)
    for dose in doses:
        for t in range(dose.shape[1] // LANES):
            d = dose[:, t * LANES : (t + 1) * LANES].astype(F32)
            folded = folded + d * d
    return jnp.sum(jnp.transpose(folded), axis=0, keepdims=True)


BLOCK = 256


def panel_stats(count, keep_ref, got_ref):
    sy, syy = row_sums((keep_ref, got_ref))
    return sy / count, lax.rsqrt(jnp.maximum(syy - sy * sy / count, 1.0))


def correlations(count, keep_ref, got_ref, dose, other, stats):
    cross = lax.dot_general(keep_ref[...], dose[...], NT, preferred_element_type=F32)
    cross = cross + lax.dot_general(got_ref[...], other[...], NT, preferred_element_type=F32)
    sx = cross[ONES : ONES + 1]
    sxx = square_sums((dose, other))
    dose_scale = lax.rsqrt(jnp.maximum(sxx - sx * sx / count, 1.0))
    mean, scale = stats
    return (cross - sx * mean) * dose_scale * scale


def streamed(blocks, dose_hbm, other_hbm, doses, sems, body):
    copies = []
    for i in range(blocks):
        rows = pl.ds(i * BLOCK, BLOCK)
        for side, source in enumerate((dose_hbm, other_hbm)):
            copy = pltpu.make_async_copy(source.at[rows], doses.at[side, i], sems.at[side, i])
            copy.start()
            copies.append(copy)
    for i in range(blocks):
        copies[2 * i].wait()
        copies[2 * i + 1].wait()
        body(i, doses.at[0, i], doses.at[1, i])


def dose_scratch(blocks, samples):
    return [
        pltpu.VMEM((2, blocks, BLOCK, samples), BF16),
        pltpu.SemaphoreType.DMA((2, blocks)),
    ]


def own_product(window_start, keep, got, dosage, other, count):
    blocks = dosage.shape[0] // BLOCK
    side = jax.ShapeDtypeStruct((ROWS, HALF), BF16)

    def kernel(
        start_ref, keep_ref, got_ref, dose_hbm, other_hbm, mine_ref, theirs_ref, doses, sems, wide
    ):
        core = lax.axis_index("samples")
        stats = []

        def body(i, dose, other):
            if i == 0:
                stats.append(panel_stats(count, keep_ref, got_ref))
            lanes = slice(i * BLOCK, (i + 1) * BLOCK)
            wide[:, lanes] = correlations(count, keep_ref, got_ref, dose, other, stats[0])

        streamed(blocks, dose_hbm, other_hbm, doses, sems, body)
        wide[:, W : W + SPILL] = jnp.zeros((ROWS, SPILL), F32)
        for ref, side in ((theirs_ref, 1 - core), (mine_ref, core)):
            last = []
            for j in range(GROUP):
                begin = start_ref[GROUP * core + j] + side * HALF
                window = pl.ds(pl.multiple_of(begin, LANES), HALF)
                rows = slice(SLOTS * j, SLOTS * j + SLOTS)
                ref[rows, :] = wide[rows, window].astype(BF16)
                last.append(wide[RATIOS + j : RATIOS + j + 1, window])
            last = jnp.concatenate(last + last, axis=0)
            ref[RATIOS:ROWS, :] = last.astype(BF16)

    return pl.pallas_call(
        kernel,
        out_shape=(side, side),
        in_specs=[SMEM, VMEM, VMEM, HBM, HBM],
        out_specs=(VMEM, VMEM),
        scratch_shapes=dose_scratch(blocks, dosage.shape[1])
        + [pltpu.VMEM((ROWS, W + SPILL), F32)],
        compiler_params=params(24),
        cost_estimate=cost(1_500_000_000, 1),
        name="own_product",
    )(window_start, keep, got, dosage, other)


def spill_product(keep, got, dosage, other, count):
    blocks = SPILL // BLOCK

    def kernel(keep_ref, got_ref, dose_hbm, other_hbm, out_ref, doses, sems):
        stats = []

        def body(i, dose, other):
            if i == 0:
                stats.append(panel_stats(count, keep_ref, got_ref))
            lanes = slice(i * BLOCK, (i + 1) * BLOCK)
            value = correlations(count, keep_ref, got_ref, dose, other, stats[0])
            out_ref[:, lanes] = value.astype(BF16)

        streamed(blocks, dose_hbm, other_hbm, doses, sems, body)

    return pl.pallas_call(
        kernel,
        out_shape=jax.ShapeDtypeStruct((ROWS, SPILL), BF16),
        in_specs=[VMEM, VMEM, HBM, HBM],
        out_specs=VMEM,
        scratch_shapes=dose_scratch(blocks, dosage.shape[1]),
        compiler_params=params(16),
        cost_estimate=cost(700_000_000, 1),
        name="spill_product",
    )(keep, got, dosage, other)


def merge_kernel(start_ref, mine_ref, other_ref, back0, back1, out_ref, wide, rows48):
    core = lax.axis_index("samples")
    back = (back0, back1)
    for c in range(2):
        wide[c, :, SPILL : 2 * SPILL] = back[c][...].astype(F32)
    for own_ref, c in ((mine_ref, core), (other_ref, 1 - core)):
        every = own_ref[...].astype(F32)
        for j in range(GROUP):
            begin = start_ref[GROUP * c + j]
            window = pl.ds(pl.multiple_of(begin, LANES), HALF)
            edge = jnp.where(core == 1, HALF - begin, HALF)
            at = 48 * (GROUP * c + j)
            for rows, to in (
                (slice(SLOTS * j, SLOTS * j + SLOTS), pl.ds(pl.multiple_of(at, 8), SLOTS)),
                (slice(RATIOS + j, RATIOS + j + 1), pl.ds(at + SLOTS, 1)),
            ):
                own = every[rows, :]
                lane = lax.broadcasted_iota(jnp.int32, own.shape, 1)
                value = jnp.where(lane >= edge, wide[c, rows, window], own)
                for t in range(HALF // LANES):
                    rows48[t, to, :] = value[:, t * LANES : (t + 1) * LANES]
    for p in range(SLOTS + 1):
        row = SLOTS if p == 0 else p - 1
        for t in range(HALF // LANES):
            genes = rows48[t, pl.ds(row, GENE_DEV, stride=48), :]
            out_ref[p, :, t * LANES : (t + 1) * LANES] = genes.astype(BF16)


def merge(window_start, mine, other, back):
    return pl.pallas_call(
        merge_kernel,
        out_shape=jax.ShapeDtypeStruct((SLOTS + 1, GENE_DEV, HALF), BF16),
        in_specs=[SMEM] + [VMEM] * 4,
        out_specs=VMEM,
        scratch_shapes=[
            pltpu.VMEM((2, ROWS, 2 * SPILL), F32),
            pltpu.VMEM((HALF // LANES, 48 * GENE_DEV, LANES), F32),
        ],
        compiler_params=params(24),
        cost_estimate=cost(2_000_000, 3_500_000),
        name="merge_windows",
    )(window_start, mine, other, *back)


def shards(dosage, expression, intron_counts, cluster_sizes, valid_mask, gene_block, window_start):
    owners = lax.axis_size("genes")
    cores = lax.axis_size("samples")
    count = float(dosage.shape[1] * cores)
    onward = [(i, i + 1) for i in range(owners - 1)]
    swap = [(i, cores - 1 - i) for i in range(cores)]
    last = cores - 1
    home = [
        [((i + 1) * cores + c, i * cores + last) for i in range(owners - 1)] for c in range(cores)
    ]
    sizes, valid = cluster_sizes.T, valid_mask.T

    def exchanged(x):
        return lax.ppermute(x, "samples", swap)

    other_dose = exchanged(dosage)
    blocks = gather_blocks(gene_block, intron_counts, owners)
    prev_expression = lax.ppermute(expression, "genes", onward)
    recv = lax.all_to_all(blocks, "genes", 0, 0, tiled=True)

    keep, give = make_panel(recv, prev_expression, sizes, valid, 1)
    got = exchanged(give)
    piece = spill_product(keep, got, dosage, other_dose, count)
    back = []
    for c in range(cores):
        back.append(lax.ppermute(piece, ("genes", "samples"), home[c]))

    keep, give = make_panel(recv, expression, sizes, valid, 0)
    got = exchanged(give)
    mine, theirs = own_product(window_start, keep, got, dosage, other_dose, count)
    other = exchanged(theirs)
    out = merge(window_start, mine, other, back)
    return jnp.transpose(out, (1, 0, 2))


def solution(mesh):
    in_specs = (
        P(("parts", "genes"), "samples"),
        P(("parts", "genes"), "samples"),
        P(("parts", "samples", "genes"), None),
        P("parts", None),
        P("parts", None),
        P("parts"),
        P(("parts", "genes")),
    )
    out_specs = P(("parts", "genes"), None, "samples")
    return jax.shard_map(shards, mesh=mesh, in_specs=in_specs, out_specs=out_specs, check_vma=False)
```

```python
import functools

import jax
import jax.numpy as jnp
from jax import lax
from jax.experimental import pallas as pl
from jax.experimental.pallas import tpu as pltpu
from jax.sharding import PartitionSpec as P


W = 2048
SLOTS = 40
CLUST = 8
SPILL = 1024
HALF = 1024
GENE_DEV = 8
GROUP = 4
LANES = 128
WIDE = 384
RATIOS = SLOTS * GROUP
ROWS = RATIOS + 8
ALL_VMEM = 67_043_328
F32 = jnp.float32
BF16 = jnp.bfloat16

VMEM = pl.BlockSpec(memory_space=pltpu.VMEM)
SMEM = pl.BlockSpec(memory_space=pltpu.SMEM)
HBM = pl.BlockSpec(memory_space=pltpu.HBM)


def params(mib):
    return pltpu.CompilerParams(vmem_limit_bytes=mib * 1024 * 1024)


def cost(flops, nbytes):
    return pl.CostEstimate(flops=flops, bytes_accessed=nbytes, transcendentals=0)


def gather_kernel(block_hbm, counts_hbm, out_ref, block_ref, counts_ref, sems):
    blocks_in = pltpu.make_async_copy(block_hbm, block_ref, sems.at[0])
    width = counts_hbm.shape[1]
    counts_in = pltpu.make_async_copy(counts_hbm, counts_ref.at[:, pl.ds(0, width)], sems.at[1])
    blocks_in.start()
    counts_in.start()
    samples = counts_ref.shape[0]
    owners = out_ref.shape[0]
    lane = lax.broadcasted_iota(jnp.int32, (samples, LANES), 1)
    low = lax.broadcasted_iota(jnp.int32, (samples // 2, LANES), 1) < 64
    out_ref[0, 0:40, :] = jnp.zeros((40, LANES), BF16)
    blocks_in.wait()
    counts_in.wait()

    def owner(o, carry):
        g = []
        for i in range(GENE_DEV):
            eighths = block_ref[o * GENE_DEV + i] * (SLOTS // 8)
            inside = (eighths & 15) * 8
            start = lax.shift_right_logical(eighths, 4) * LANES
            pair = counts_ref[:, pl.ds(pl.multiple_of(start, LANES), 2 * LANES)].astype(F32)
            both = jnp.where(lane >= inside, pair[:, :LANES], pair[:, LANES:])
            g.append(pltpu.roll(both, (SLOTS * i - inside) & (LANES - 1), 1))
        a = jnp.where(lane < 40, g[0], jnp.where(lane < 80, g[1], jnp.where(lane < 120, g[2], g[3])))
        b = jnp.where(lane < 32, g[3], jnp.where(lane < 72, g[4], jnp.where(lane < 112, g[5], g[6])))
        c = jnp.where(lane < 24, g[6], g[7])
        packed = jnp.where(low, c[: samples // 2], pltpu.roll(c[samples // 2 :], 64, 1))
        after = jnp.minimum(o + 1, owners - 1)
        for at, row in ((after, 0), (o, 40)):
            out_ref[at, row : row + 16, :] = a.astype(BF16)
            out_ref[at, row + 16 : row + 32, :] = b.astype(BF16)
            out_ref[at, row + 32 : row + 40, :] = packed.astype(BF16)
        return carry

    owner(owners - 1, 0)
    lax.fori_loop(0, owners - 1, owner, 0, unroll=9)


def gather_blocks(gene_block, counts, owners):
    return pl.pallas_call(
        gather_kernel,
        out_shape=jax.ShapeDtypeStruct((owners, 80, LANES), BF16),
        in_specs=[HBM, HBM],
        out_specs=VMEM,
        scratch_shapes=[
            pltpu.SMEM(gene_block.shape, jnp.int32),
            pltpu.VMEM((counts.shape[0], counts.shape[1] + LANES), BF16),
            pltpu.SemaphoreType.DMA((2,)),
        ],
        compiler_params=pltpu.CompilerParams(vmem_limit_bytes=ALL_VMEM),
        cost_estimate=cost(10_000_000, 1),
        name="gather_blocks",
    )(gene_block, counts)


def panel_kernel(behind, recv_ref, expr_ref, sizes_ref, valid_ref, *refs):
    hbm, (keep_ref, give_ref), kept, sems = refs[:2], refs[2:4], refs[4:6], refs[6]
    rows = pl.ds((1 - behind) * SPILL, SPILL)
    copies = [
        pltpu.make_async_copy(source.at[rows], to, sems.at[side])
        for side, (source, to) in enumerate(zip(hbm, kept))
    ]
    for copy in copies:
        copy.start()
    me = jnp.maximum(lax.axis_index("genes") - behind, 0)
    first_core = lax.axis_index("samples") == 0
    first = me * GENE_DEV
    start = pl.multiple_of(first // LANES * LANES, LANES)
    back = (LANES - first % LANES) & (LANES - 1)
    sizes = pltpu.roll(sizes_ref[:, pl.ds(start, LANES)].astype(F32), back, 1)
    valid = pltpu.roll(valid_ref[:, pl.ds(start, LANES)].astype(F32), back, 1)
    ends, running = [], jnp.zeros((1, LANES), F32)
    for c in range(CLUST):
        running = running + sizes[c : c + 1, :]
        ends.append(running)
    ends = jnp.concatenate(ends, axis=0)

    x = lax.broadcasted_iota(jnp.int32, (LANES, WIDE), 1)
    i = lax.broadcasted_iota(jnp.int32, (LANES, WIDE), 0)
    spread = jnp.where((x >= SLOTS * i) & (x < SLOTS * i + SLOTS) & (i < GENE_DEV), 1.0, 0.0)
    spread = spread.astype(BF16)

    def slots_of(rows):
        x = lax.broadcasted_iota(jnp.int32, (rows, WIDE), 1)
        base = jnp.zeros((rows, WIDE), jnp.int32)
        for gene in range(1, GENE_DEV + 1):
            base = jnp.where(x >= SLOTS * gene, SLOTS * gene, base)
        return base, x - base

    ends_at = jnp.dot(ends.astype(BF16), spread, preferred_element_type=F32)
    base, slot = slots_of(CLUST)
    slot = slot.astype(F32)
    low = jnp.max(jnp.where(ends_at <= slot, ends_at, 0.0), axis=0, keepdims=True)
    high = jnp.min(jnp.where(ends_at > slot, ends_at, float(SLOTS)), axis=0, keepdims=True)
    base = base[0:1, :].astype(F32)
    valid_at = jnp.dot(valid.astype(BF16), spread, preferred_element_type=F32)
    _, slot40 = slots_of(SLOTS)
    row40 = lax.broadcasted_iota(jnp.int32, (SLOTS, WIDE), 0)
    live = jnp.sum(jnp.where(slot40 == row40, valid_at, 0.0), axis=0, keepdims=True)

    k = lax.broadcasted_iota(jnp.int32, (WIDE, WIDE), 0).astype(F32)
    inside = (k >= base + low) & (k < base + high)
    same = jnp.where(inside & (k < float(SLOTS * GENE_DEV)), 1.0, 0.0).astype(BF16)

    per = LANES // 16
    for t in range(recv_ref.shape[0] // per):
        owned = 40 * (1 - behind)
        piece = recv_ref[t * per : (t + 1) * per, owned : owned + 40, :].astype(F32)
        a = piece[:, 0:16, :].reshape(LANES, LANES)
        b = piece[:, 16:32, :].reshape(LANES, LANES)
        c = piece[:, 32:40, :]
        swapped = pltpu.roll(c, 64, 2)
        c = jnp.concatenate([c, swapped], axis=1).reshape(LANES, LANES)
        counts = jnp.concatenate([a, b, c], axis=1) * live
        total = jnp.dot(counts.astype(BF16), same, preferred_element_type=F32)
        ratio = counts / jnp.maximum(total, 1.0)
        lanes = slice(t * LANES, (t + 1) * LANES)
        turned = jnp.transpose(ratio)
        low_half, high_half = turned[0:RATIOS], turned[RATIOS : 2 * RATIOS]
        keep_ref[0:RATIOS, lanes] = jnp.where(first_core, low_half, high_half).astype(BF16)
        give_ref[0:RATIOS, lanes] = jnp.where(first_core, high_half, low_half).astype(BF16)
    expr = expr_ref[...].astype(F32)
    row = lax.broadcasted_iota(jnp.int32, expr.shape, 0)
    low_half = jnp.where(row < GROUP, expr, 1.0)
    high_half = jnp.where(row < GROUP, pltpu.roll(expr, GROUP, 0), 1.0)
    keep_ref[RATIOS:ROWS, :] = jnp.where(first_core, low_half, high_half).astype(BF16)
    give_ref[RATIOS:ROWS, :] = jnp.where(first_core, high_half, low_half).astype(BF16)
    for copy in copies:
        copy.wait()


def make_panel(recv, expression, sizes, valid, doses, behind, limit):
    samples = expression.shape[1]
    half = jax.ShapeDtypeStruct((ROWS, samples), BF16)
    rows = jax.ShapeDtypeStruct((SPILL, samples), BF16)
    return pl.pallas_call(
        functools.partial(panel_kernel, behind),
        out_shape=(half, half, rows, rows),
        in_specs=[VMEM] * 4 + [HBM, HBM],
        out_specs=(VMEM,) * 4,
        scratch_shapes=[pltpu.SemaphoreType.DMA((2,))],
        compiler_params=params(limit),
        cost_estimate=cost(400_000_000, 6_000_000),
        name="make_panel",
    )(recv, expression, sizes, valid, *doses)


NT = (((1,), (1,)), ((), ()))


def row_sums(panels):
    rows = panels[0].shape[0]
    one, two = jnp.zeros((rows, LANES), F32), jnp.zeros((rows, LANES), F32)
    for panel in panels:
        for t in range(panel.shape[1] // LANES):
            p = panel[:, t * LANES : (t + 1) * LANES].astype(F32)
            one, two = one + p, two + p * p
    return jnp.sum(one, axis=1, keepdims=True), jnp.sum(two, axis=1, keepdims=True)


def dose_kernel(count, dose_ref, other_ref, stats_ref):
    block = dose_ref.shape[0]
    one, two = jnp.zeros((block, LANES), F32), jnp.zeros((block, LANES), F32)
    for ref in (dose_ref, other_ref):
        for t in range(ref.shape[1] // LANES):
            d = ref[:, t * LANES : (t + 1) * LANES].astype(F32)
            one, two = one + d, two + d * d
    sx = jnp.sum(jnp.transpose(one), axis=0, keepdims=True)
    sxx = jnp.sum(jnp.transpose(two), axis=0, keepdims=True)
    scale = lax.rsqrt(jnp.maximum(sxx - sx * sx / count, 1.0))
    row = lax.broadcasted_iota(jnp.int32, (8, block), 0)
    stats_ref[...] = jnp.where(row == 0, sx, scale)


def dose_stats(dosage, other, count):
    rows, samples = dosage.shape
    block = 256
    spec = pl.BlockSpec((block, samples), lambda i: (i, 0))
    return pl.pallas_call(
        functools.partial(dose_kernel, count),
        grid=(rows // block,),
        out_shape=jax.ShapeDtypeStruct((8, rows), F32),
        in_specs=[spec, spec],
        out_specs=pl.BlockSpec((8, block), lambda i: (0, i)),
        compiler_params=params(8),
        cost_estimate=cost(20_000_000, 16_000_000),
        name="dose_stats",
    )(dosage, other)


BLOCK = 256


def correlations(count, keep_ref, got_ref, stats_ref, doses, put):
    sy, syy = row_sums((keep_ref, got_ref))
    mean = sy / count
    scale = lax.rsqrt(jnp.maximum(syy - sy * mean, 1.0))
    per = SPILL // BLOCK
    for i in range(per * len(doses)):
        dose_ref, other_ref = doses[i // per]
        rows = slice(i % per * BLOCK, (i % per + 1) * BLOCK)
        lanes = slice(i * BLOCK, (i + 1) * BLOCK)
        cross = lax.dot_general(keep_ref[...], dose_ref[rows], NT, preferred_element_type=F32)
        cross = cross + lax.dot_general(
            got_ref[...], other_ref[rows], NT, preferred_element_type=F32
        )
        put(lanes, (cross - stats_ref[0:1, lanes] * mean) * stats_ref[1:2, lanes] * scale)


def own_product(window_start, keep, got, stats, near, far, count):
    side = jax.ShapeDtypeStruct((ROWS, HALF), BF16)

    def kernel(start_ref, keep_ref, got_ref, stats_ref, *refs):
        doses, (mine_ref, theirs_ref, wide) = (refs[0:2], refs[2:4]), refs[4:]
        core = lax.axis_index("samples")

        def put(lanes, values):
            wide[:, lanes] = values

        correlations(count, keep_ref, got_ref, stats_ref, doses, put)
        wide[:, W : W + SPILL] = jnp.zeros((ROWS, SPILL), F32)
        for ref, side in ((theirs_ref, 1 - core), (mine_ref, core)):
            last = []
            for j in range(GROUP):
                begin = start_ref[GROUP * core + j] + side * HALF
                window = pl.ds(pl.multiple_of(begin, LANES), HALF)
                rows = slice(SLOTS * j, SLOTS * j + SLOTS)
                ref[rows, :] = wide[rows, window].astype(BF16)
                last.append(wide[RATIOS + j : RATIOS + j + 1, window])
            last = jnp.concatenate(last + last, axis=0)
            ref[RATIOS:ROWS, :] = last.astype(BF16)

    return pl.pallas_call(
        kernel,
        out_shape=(side, side),
        in_specs=[SMEM] + [VMEM] * 7,
        out_specs=(VMEM, VMEM),
        scratch_shapes=[pltpu.VMEM((ROWS, W + SPILL), F32)],
        compiler_params=params(16),
        cost_estimate=cost(1_500_000_000, 12_000_000),
        name="own_product",
    )(window_start, keep, got, stats, *near, *far)


def spill_product(keep, got, stats, near, count):
    def kernel(keep_ref, got_ref, stats_ref, dose_ref, other_ref, out_ref):
        def put(lanes, values):
            out_ref[:, lanes] = values.astype(BF16)

        correlations(count, keep_ref, got_ref, stats_ref, ((dose_ref, other_ref),), put)

    return pl.pallas_call(
        kernel,
        out_shape=jax.ShapeDtypeStruct((ROWS, SPILL), BF16),
        in_specs=[VMEM] * 5,
        out_specs=VMEM,
        compiler_params=params(16),
        cost_estimate=cost(700_000_000, 6_000_000),
        name="spill_product",
    )(keep, got, stats, *near)


def merge_kernel(start_ref, mine_ref, other_ref, back0, back1, out_ref, wide, rows48):
    core = lax.axis_index("samples")
    back = (back0, back1)
    for c in range(2):
        wide[c, :, SPILL : 2 * SPILL] = back[c][...].astype(F32)
    for own_ref, c in ((mine_ref, core), (other_ref, 1 - core)):
        every = own_ref[...].astype(F32)
        for j in range(GROUP):
            begin = start_ref[GROUP * c + j]
            window = pl.ds(pl.multiple_of(begin, LANES), HALF)
            edge = jnp.where(core == 1, HALF - begin, HALF)
            at = 48 * (GROUP * c + j)
            for rows, to in (
                (slice(SLOTS * j, SLOTS * j + SLOTS), pl.ds(pl.multiple_of(at, 8), SLOTS)),
                (slice(RATIOS + j, RATIOS + j + 1), pl.ds(at + SLOTS, 1)),
            ):
                own = every[rows, :]
                lane = lax.broadcasted_iota(jnp.int32, own.shape, 1)
                value = jnp.where(lane >= edge, wide[c, rows, window], own)
                for t in range(HALF // LANES):
                    rows48[t, to, :] = value[:, t * LANES : (t + 1) * LANES]
    for p in range(SLOTS + 1):
        row = SLOTS if p == 0 else p - 1
        for t in range(HALF // LANES):
            genes = rows48[t, pl.ds(row, GENE_DEV, stride=48), :]
            out_ref[p, :, t * LANES : (t + 1) * LANES] = genes.astype(BF16)


def merge(window_start, mine, other, back):
    return pl.pallas_call(
        merge_kernel,
        out_shape=jax.ShapeDtypeStruct((SLOTS + 1, GENE_DEV, HALF), BF16),
        in_specs=[SMEM] + [VMEM] * 4,
        out_specs=VMEM,
        scratch_shapes=[
            pltpu.VMEM((2, ROWS, 2 * SPILL), F32),
            pltpu.VMEM((HALF // LANES, 48 * GENE_DEV, LANES), F32),
        ],
        compiler_params=params(24),
        cost_estimate=cost(2_000_000, 3_500_000),
        name="merge_windows",
    )(window_start, mine, other, *back)


def shards(dosage, expression, intron_counts, cluster_sizes, valid_mask, gene_block, window_start):
    owners = lax.axis_size("genes")
    cores = lax.axis_size("samples")
    count = float(dosage.shape[1] * cores)
    onward = [(i, i + 1) for i in range(owners - 1)]
    swap = [(i, cores - 1 - i) for i in range(cores)]
    last = cores - 1
    home = [
        [((i + 1) * cores + c, i * cores + last) for i in range(owners - 1)] for c in range(cores)
    ]
    sizes, valid = cluster_sizes.T, valid_mask.T

    def exchanged(x):
        return lax.ppermute(x, "samples", swap)

    other_dose = exchanged(dosage)
    blocks = gather_blocks(gene_block, intron_counts, owners)
    prev_expression = lax.ppermute(expression, "genes", onward)
    recv = lax.all_to_all(blocks, "genes", 0, 0, tiled=True)

    stats = dose_stats(dosage, other_dose, count)
    doses = (dosage, other_dose)

    keep, give, *near = make_panel(recv, prev_expression, sizes, valid, doses, 1, 44)
    got = exchanged(give)
    piece = spill_product(keep, got, stats, near, count)
    back = []
    for c in range(cores):
        back.append(lax.ppermute(piece, ("genes", "samples"), home[c]))

    keep, give, *far = make_panel(recv, expression, sizes, valid, doses, 0, 40)
    got = exchanged(give)
    mine, theirs = own_product(window_start, keep, got, stats, near, far, count)
    other = exchanged(theirs)
    out = merge(window_start, mine, other, back)
    return jnp.transpose(out, (1, 0, 2))


def solution(mesh):
    in_specs = (
        P(("parts", "genes"), "samples"),
        P(("parts", "genes"), "samples"),
        P(("parts", "samples", "genes"), None),
        P("parts", None),
        P("parts", None),
        P("parts"),
        P(("parts", "genes")),
    )
    out_specs = P(("parts", "genes"), None, "samples")
    return jax.shard_map(shards, mesh=mesh, in_specs=in_specs, out_specs=out_specs, check_vma=False)
```

```python
import functools

import jax
import jax.numpy as jnp
from jax import lax
from jax.experimental import pallas as pl
from jax.experimental.pallas import tpu as pltpu
from jax.sharding import PartitionSpec as P


W = 2048
SLOTS = 40
CLUST = 8
SPILL = 1024
HALF = 1024
GENE_DEV = 8
GROUP = 4
LANES = 128
WIDE = 384
RATIOS = SLOTS * GROUP
ROWS = RATIOS + 8
ALL_VMEM = 67_043_328
LIM = 44
F32 = jnp.float32
BF16 = jnp.bfloat16

VMEM = pl.BlockSpec(memory_space=pltpu.VMEM)
SMEM = pl.BlockSpec(memory_space=pltpu.SMEM)
HBM = pl.BlockSpec(memory_space=pltpu.HBM)


def params(mib):
    return pltpu.CompilerParams(vmem_limit_bytes=mib * 1024 * 1024)


def cost(flops, nbytes):
    return pl.CostEstimate(flops=flops, bytes_accessed=nbytes, transcendentals=0)


def gather_kernel(block_hbm, counts_hbm, out_ref, block_ref, counts_ref, sems):
    blocks_in = pltpu.make_async_copy(block_hbm, block_ref, sems.at[0])
    width = counts_hbm.shape[1]
    counts_in = pltpu.make_async_copy(counts_hbm, counts_ref.at[:, pl.ds(0, width)], sems.at[1])
    blocks_in.start()
    counts_in.start()
    samples = counts_ref.shape[0]
    lane = lax.broadcasted_iota(jnp.int32, (samples, LANES), 1)
    low = lax.broadcasted_iota(jnp.int32, (samples // 2, LANES), 1) < 64
    blocks_in.wait()
    counts_in.wait()

    def owner(o, carry):
        g = []
        for i in range(GENE_DEV):
            eighths = block_ref[o * GENE_DEV + i] * (SLOTS // 8)
            inside = (eighths & 15) * 8
            start = lax.shift_right_logical(eighths, 4) * LANES
            pair = counts_ref[:, pl.ds(pl.multiple_of(start, LANES), 2 * LANES)].astype(F32)
            both = jnp.where(lane >= inside, pair[:, :LANES], pair[:, LANES:])
            g.append(pltpu.roll(both, (SLOTS * i - inside) & (LANES - 1), 1))
        a = jnp.where(lane < 40, g[0], jnp.where(lane < 80, g[1], jnp.where(lane < 120, g[2], g[3])))
        b = jnp.where(lane < 32, g[3], jnp.where(lane < 72, g[4], jnp.where(lane < 112, g[5], g[6])))
        c = jnp.where(lane < 24, g[6], g[7])
        packed = jnp.where(low, c[: samples // 2], pltpu.roll(c[samples // 2 :], 64, 1))
        out_ref[o, 0:16, :] = a.astype(BF16)
        out_ref[o, 16:32, :] = b.astype(BF16)
        out_ref[o, 32:40, :] = packed.astype(BF16)
        return carry

    lax.fori_loop(0, out_ref.shape[0], owner, 0, unroll=8)


def gather_blocks(gene_block, counts, owners):
    return pl.pallas_call(
        gather_kernel,
        out_shape=jax.ShapeDtypeStruct((owners, 40, LANES), BF16),
        in_specs=[HBM, HBM],
        out_specs=VMEM,
        scratch_shapes=[
            pltpu.SMEM(gene_block.shape, jnp.int32),
            pltpu.VMEM((counts.shape[0], counts.shape[1] + LANES), BF16),
            pltpu.SemaphoreType.DMA((2,)),
        ],
        compiler_params=pltpu.CompilerParams(vmem_limit_bytes=ALL_VMEM),
        cost_estimate=cost(10_000_000, 1),
        name="gather_blocks",
    )(gene_block, counts)


def tables_kernel(expr_ref, sizes_ref, valid_ref, same_ref, live_ref, kept_ref):
    kept_ref[...] = expr_ref[...]
    me = lax.axis_index("genes")
    first = me * GENE_DEV
    start = pl.multiple_of(first // LANES * LANES, LANES)
    back = (LANES - first % LANES) & (LANES - 1)
    sizes = pltpu.roll(sizes_ref[:, pl.ds(start, LANES)].astype(F32), back, 1)
    valid = pltpu.roll(valid_ref[:, pl.ds(start, LANES)].astype(F32), back, 1)
    ends, running = [], jnp.zeros((1, LANES), F32)
    for c in range(CLUST):
        running = running + sizes[c : c + 1, :]
        ends.append(running)
    ends = jnp.concatenate(ends, axis=0)

    x = lax.broadcasted_iota(jnp.int32, (LANES, WIDE), 1)
    i = lax.broadcasted_iota(jnp.int32, (LANES, WIDE), 0)
    spread = jnp.where((x >= SLOTS * i) & (x < SLOTS * i + SLOTS) & (i < GENE_DEV), 1.0, 0.0)
    spread = spread.astype(BF16)

    def slots_of(rows):
        x = lax.broadcasted_iota(jnp.int32, (rows, WIDE), 1)
        base = jnp.zeros((rows, WIDE), jnp.int32)
        for gene in range(1, GENE_DEV + 1):
            base = jnp.where(x >= SLOTS * gene, SLOTS * gene, base)
        return base, x - base

    ends_at = jnp.dot(ends.astype(BF16), spread, preferred_element_type=F32)
    base, slot = slots_of(CLUST)
    slot = slot.astype(F32)
    low = jnp.max(jnp.where(ends_at <= slot, ends_at, 0.0), axis=0, keepdims=True)
    high = jnp.min(jnp.where(ends_at > slot, ends_at, float(SLOTS)), axis=0, keepdims=True)
    base = base[0:1, :].astype(F32)
    valid_at = jnp.dot(valid.astype(BF16), spread, preferred_element_type=F32)
    _, slot40 = slots_of(SLOTS)
    row40 = lax.broadcasted_iota(jnp.int32, (SLOTS, WIDE), 0)
    live = jnp.sum(jnp.where(slot40 == row40, valid_at, 0.0), axis=0, keepdims=True)

    k = lax.broadcasted_iota(jnp.int32, (WIDE, WIDE), 0).astype(F32)
    inside = (k >= base + low) & (k < base + high)
    same_ref[...] = jnp.where(inside & (k < float(SLOTS * GENE_DEV)), 1.0, 0.0).astype(BF16)
    live_ref[...] = jnp.broadcast_to(live, (8, WIDE))


def make_tables(expression, sizes, valid):
    return pl.pallas_call(
        tables_kernel,
        out_shape=(
            jax.ShapeDtypeStruct((WIDE, WIDE), BF16),
            jax.ShapeDtypeStruct((8, WIDE), F32),
            jax.ShapeDtypeStruct(expression.shape, expression.dtype),
        ),
        in_specs=[VMEM] * 3,
        out_specs=(VMEM,) * 3,
        compiler_params=params(16),
        cost_estimate=cost(10_000_000, 1_000_000),
        name="make_tables",
    )(expression, sizes, valid)


def panel_kernel(recv_ref, same_ref, live_ref, expr_ref, keep_ref, give_ref):
    first_core = lax.axis_index("samples") == 0
    live = live_ref[0:1, :]
    same = same_ref[...]
    per = LANES // 16
    for t in range(recv_ref.shape[0] // per):
        piece = recv_ref[t * per : (t + 1) * per].astype(F32)
        a = piece[:, 0:16, :].reshape(LANES, LANES)
        b = piece[:, 16:32, :].reshape(LANES, LANES)
        c = piece[:, 32:40, :]
        swapped = pltpu.roll(c, 64, 2)
        c = jnp.concatenate([c, swapped], axis=1).reshape(LANES, LANES)
        counts = jnp.concatenate([a, b, c], axis=1) * live
        total = jnp.dot(counts.astype(BF16), same, preferred_element_type=F32)
        ratio = counts / jnp.maximum(total, 1.0)
        lanes = slice(t * LANES, (t + 1) * LANES)
        turned = jnp.transpose(ratio)
        low_half, high_half = turned[0:RATIOS], turned[RATIOS : 2 * RATIOS]
        keep_ref[0:RATIOS, lanes] = jnp.where(first_core, low_half, high_half).astype(BF16)
        give_ref[0:RATIOS, lanes] = jnp.where(first_core, high_half, low_half).astype(BF16)
    expr = expr_ref[...].astype(F32)
    row = lax.broadcasted_iota(jnp.int32, expr.shape, 0)
    low_half = jnp.where(row < GROUP, expr, 1.0)
    high_half = jnp.where(row < GROUP, pltpu.roll(expr, GROUP, 0), 1.0)
    keep_ref[RATIOS:ROWS, :] = jnp.where(first_core, low_half, high_half).astype(BF16)
    give_ref[RATIOS:ROWS, :] = jnp.where(first_core, high_half, low_half).astype(BF16)


def make_panel(recv, tables):
    half = jax.ShapeDtypeStruct((ROWS, tables[2].shape[1]), BF16)
    return pl.pallas_call(
        panel_kernel,
        out_shape=(half, half),
        in_specs=[VMEM] * 4,
        out_specs=(VMEM, VMEM),
        compiler_params=params(16),
        cost_estimate=cost(400_000_000, 2_000_000),
        name="make_panel",
    )(recv, *tables)


NT = (((1,), (1,)), ((), ()))


def row_sums(panels):
    rows = panels[0].shape[0]
    one, two = jnp.zeros((rows, LANES), F32), jnp.zeros((rows, LANES), F32)
    for panel in panels:
        for t in range(panel.shape[1] // LANES):
            p = panel[:, t * LANES : (t + 1) * LANES].astype(F32)
            one, two = one + p, two + p * p
    return jnp.sum(one, axis=1, keepdims=True), jnp.sum(two, axis=1, keepdims=True)


BLOCK = 256


def dose_kernel(count, dose_hbm, other_hbm, dose_ref, other_ref, stats_ref, sems):
    blocks = dose_ref.shape[0] // BLOCK
    copies = [
        [
            pltpu.make_async_copy(
                source.at[pl.ds(i * BLOCK, BLOCK)], to.at[pl.ds(i * BLOCK, BLOCK)], sems.at[side, i]
            )
            for side, (source, to) in enumerate(((dose_hbm, dose_ref), (other_hbm, other_ref)))
        ]
        for i in range(blocks)
    ]
    for pair in copies:
        for copy in pair:
            copy.start()
    row = lax.broadcasted_iota(jnp.int32, (8, BLOCK), 0)
    for i, pair in enumerate(copies):
        one, two = jnp.zeros((BLOCK, LANES), F32), jnp.zeros((BLOCK, LANES), F32)
        for copy, ref in zip(pair, (dose_ref, other_ref)):
            copy.wait()
            for t in range(ref.shape[1] // LANES):
                d = ref[i * BLOCK : (i + 1) * BLOCK, t * LANES : (t + 1) * LANES].astype(F32)
                one, two = one + d, two + d * d
        sx = jnp.sum(jnp.transpose(one), axis=0, keepdims=True)
        sxx = jnp.sum(jnp.transpose(two), axis=0, keepdims=True)
        scale = lax.rsqrt(jnp.maximum(sxx - sx * sx / count, 1.0))
        stats_ref[:, i * BLOCK : (i + 1) * BLOCK] = jnp.where(row == 0, sx, scale)


def dose_stats(dosage, other, count):
    rows = dosage.shape[0]
    same = jax.ShapeDtypeStruct(dosage.shape, dosage.dtype)
    return pl.pallas_call(
        functools.partial(dose_kernel, count),
        out_shape=(same, same, jax.ShapeDtypeStruct((8, rows), F32)),
        in_specs=[HBM, HBM],
        out_specs=(VMEM,) * 3,
        scratch_shapes=[pltpu.SemaphoreType.DMA((2, rows // BLOCK))],
        compiler_params=params(LIM),
        cost_estimate=cost(20_000_000, 16_000_000),
        name="dose_stats",
    )(dosage, other)


def correlations(count, keep_ref, got_ref, stats_ref, doses, variants, put):
    sy, syy = row_sums((keep_ref, got_ref))
    mean = sy / count
    scale = lax.rsqrt(jnp.maximum(syy - sy * mean, 1.0))
    dose_ref, other_ref = doses
    for i in range(variants // BLOCK):
        lanes = slice(i * BLOCK, (i + 1) * BLOCK)
        cross = lax.dot_general(keep_ref[...], dose_ref[lanes], NT, preferred_element_type=F32)
        cross = cross + lax.dot_general(
            got_ref[...], other_ref[lanes], NT, preferred_element_type=F32
        )
        put(lanes, (cross - stats_ref[0:1, lanes] * mean) * stats_ref[1:2, lanes] * scale)


def own_product(window_start, keep, got, stats, doses, count):
    side = jax.ShapeDtypeStruct((ROWS, HALF), BF16)

    def kernel(start_ref, keep_ref, got_ref, stats_ref, *refs):
        doses, (mine_ref, theirs_ref, wide) = refs[:2], refs[2:]
        core = lax.axis_index("samples")

        def put(lanes, values):
            wide[:, lanes] = values

        correlations(count, keep_ref, got_ref, stats_ref, doses, W, put)
        wide[:, W : W + SPILL] = jnp.zeros((ROWS, SPILL), F32)
        for ref, side in ((theirs_ref, 1 - core), (mine_ref, core)):
            last = []
            for j in range(GROUP):
                begin = start_ref[GROUP * core + j] + side * HALF
                window = pl.ds(pl.multiple_of(begin, LANES), HALF)
                rows = slice(SLOTS * j, SLOTS * j + SLOTS)
                ref[rows, :] = wide[rows, window].astype(BF16)
                last.append(wide[RATIOS + j : RATIOS + j + 1, window])
            last = jnp.concatenate(last + last, axis=0)
            ref[RATIOS:ROWS, :] = last.astype(BF16)

    return pl.pallas_call(
        kernel,
        out_shape=(side, side),
        in_specs=[SMEM] + [VMEM] * 5,
        out_specs=(VMEM, VMEM),
        scratch_shapes=[pltpu.VMEM((ROWS, W + SPILL), F32)],
        compiler_params=params(16),
        cost_estimate=cost(1_500_000_000, 12_000_000),
        name="own_product",
    )(window_start, keep, got, stats, *doses)


def spill_product(keep, got, stats, doses, count):
    def kernel(keep_ref, got_ref, stats_ref, dose_ref, other_ref, out_ref):
        def put(lanes, values):
            out_ref[:, lanes] = values.astype(BF16)

        correlations(
            count, keep_ref, got_ref, stats_ref, (dose_ref, other_ref), SPILL, put
        )

    return pl.pallas_call(
        kernel,
        out_shape=jax.ShapeDtypeStruct((ROWS, SPILL), BF16),
        in_specs=[VMEM] * 5,
        out_specs=VMEM,
        compiler_params=params(16),
        cost_estimate=cost(700_000_000, 6_000_000),
        name="spill_product",
    )(keep, got, stats, *doses)


def merge_kernel(start_ref, mine_ref, other_ref, back0, back1, out_hbm, wide, rows48, out_ref, sems):
    core = lax.axis_index("samples")
    back = (back0, back1)
    for c in range(2):
        wide[c, :, SPILL : 2 * SPILL] = back[c][...].astype(F32)
    for own_ref, c in ((mine_ref, core), (other_ref, 1 - core)):
        every = own_ref[...].astype(F32)
        for j in range(GROUP):
            begin = start_ref[GROUP * c + j]
            window = pl.ds(pl.multiple_of(begin, LANES), HALF)
            edge = jnp.where(core == 1, HALF - begin, HALF)
            at = 48 * (GROUP * c + j)
            for rows, to in (
                (slice(SLOTS * j, SLOTS * j + SLOTS), pl.ds(pl.multiple_of(at, 8), SLOTS)),
                (slice(RATIOS + j, RATIOS + j + 1), pl.ds(at + SLOTS, 1)),
            ):
                own = every[rows, :]
                lane = lax.broadcasted_iota(jnp.int32, own.shape, 1)
                value = jnp.where(lane >= edge, wide[c, rows, window], own)
                for t in range(HALF // LANES):
                    rows48[t, to, :] = value[:, t * LANES : (t + 1) * LANES]
    copies = []
    for k, first in enumerate(range(0, SLOTS + 1, PIECE)):
        end = min(first + PIECE, SLOTS + 1)
        for p in range(first, end):
            row = SLOTS if p == 0 else p - 1
            for t in range(HALF // LANES):
                genes = rows48[t, pl.ds(row, GENE_DEV, stride=48), :]
                out_ref[p, :, t * LANES : (t + 1) * LANES] = genes.astype(BF16)
        part = pl.ds(first, end - first)
        copies.append(pltpu.make_async_copy(out_ref.at[part], out_hbm.at[part], sems.at[k]))
        copies[-1].start()
    for copy in copies:
        copy.wait()


PIECE = 11


def merge(window_start, mine, other, back):
    return pl.pallas_call(
        merge_kernel,
        out_shape=jax.ShapeDtypeStruct((SLOTS + 1, GENE_DEV, HALF), BF16),
        in_specs=[SMEM] + [VMEM] * 4,
        out_specs=HBM,
        scratch_shapes=[
            pltpu.VMEM((2, ROWS, 2 * SPILL), F32),
            pltpu.VMEM((HALF // LANES, 48 * GENE_DEV, LANES), F32),
            pltpu.VMEM((SLOTS + 1, GENE_DEV, HALF), BF16),
            pltpu.SemaphoreType.DMA((pl.cdiv(SLOTS + 1, PIECE),)),
        ],
        compiler_params=params(24),
        cost_estimate=cost(2_000_000, 3_500_000),
        name="merge_windows",
    )(window_start, mine, other, *back)


def shards(dosage, expression, intron_counts, cluster_sizes, valid_mask, gene_block, window_start):
    owners = lax.axis_size("genes")
    cores = lax.axis_size("samples")
    count = float(dosage.shape[1] * cores)
    onward = [(i, i + 1) for i in range(owners - 1)]
    swap = [(i, cores - 1 - i) for i in range(cores)]
    last = cores - 1
    home = [
        [((i + 1) * cores + c, i * cores + last) for i in range(owners - 1)] for c in range(cores)
    ]
    sizes, valid = cluster_sizes.T, valid_mask.T

    def exchanged(x):
        return lax.ppermute(x, "samples", swap)

    other_dose = exchanged(dosage)
    blocks = gather_blocks(gene_block, intron_counts, owners)
    recv = lax.all_to_all(blocks, "genes", 0, 0, tiled=True)
    tables = make_tables(expression, sizes, valid)
    *doses, stats = dose_stats(dosage, other_dose, count)

    keep, give = make_panel(recv, tables)
    got = exchanged(give)
    passed_keep = lax.ppermute(keep, "genes", onward)
    passed_got = lax.ppermute(got, "genes", onward)
    mine, theirs = own_product(window_start, keep, got, stats, doses, count)
    other = exchanged(theirs)

    piece = spill_product(passed_keep, passed_got, stats, doses, count)
    back = []
    for c in range(cores):
        back.append(lax.ppermute(piece, ("genes", "samples"), home[c]))
    out = merge(window_start, mine, other, back)
    return jnp.transpose(out, (1, 0, 2))


def solution(mesh):
    in_specs = (
        P(("parts", "genes"), "samples"),
        P(("parts", "genes"), "samples"),
        P(("parts", "samples", "genes"), None),
        P("parts", None),
        P("parts", None),
        P("parts"),
        P(("parts", "genes")),
    )
    out_specs = P(("parts", "genes"), None, "samples")
    return jax.shard_map(shards, mesh=mesh, in_specs=in_specs, out_specs=out_specs, check_vma=False)
```

```python
import functools

import jax
import jax.numpy as jnp
from jax import lax
from jax.experimental import pallas as pl
from jax.experimental.pallas import tpu as pltpu
from jax.sharding import PartitionSpec as P


W = 2048
SLOTS = 40
CLUST = 8
SPILL = 1024
HALF = 1024
GENE_DEV = 8
GROUP = 4
LANES = 128
WIDE = 384
RATIOS = SLOTS * GROUP
ROWS = RATIOS + 8
ALL_VMEM = 67_043_328
LIM = 44
F32 = jnp.float32
BF16 = jnp.bfloat16

VMEM = pl.BlockSpec(memory_space=pltpu.VMEM)
SMEM = pl.BlockSpec(memory_space=pltpu.SMEM)
HBM = pl.BlockSpec(memory_space=pltpu.HBM)


def params(mib):
    return pltpu.CompilerParams(vmem_limit_bytes=mib * 1024 * 1024)


def cost(flops, nbytes):
    return pl.CostEstimate(flops=flops, bytes_accessed=nbytes, transcendentals=0)


def gather_kernel(block_hbm, counts_hbm, out_ref, block_ref, counts_ref, sems):
    blocks_in = pltpu.make_async_copy(block_hbm, block_ref, sems.at[0])
    width = counts_hbm.shape[1]
    counts_in = pltpu.make_async_copy(counts_hbm, counts_ref.at[:, pl.ds(0, width)], sems.at[1])
    blocks_in.start()
    counts_in.start()
    samples = counts_ref.shape[0]
    lane = lax.broadcasted_iota(jnp.int32, (samples, LANES), 1)
    low = lax.broadcasted_iota(jnp.int32, (samples // 2, LANES), 1) < 64
    blocks_in.wait()
    counts_in.wait()

    def owner(o, carry):
        g = []
        for i in range(GENE_DEV):
            eighths = block_ref[o * GENE_DEV + i] * (SLOTS // 8)
            inside = (eighths & 15) * 8
            start = lax.shift_right_logical(eighths, 4) * LANES
            pair = counts_ref[:, pl.ds(pl.multiple_of(start, LANES), 2 * LANES)].astype(F32)
            both = jnp.where(lane >= inside, pair[:, :LANES], pair[:, LANES:])
            g.append(pltpu.roll(both, (SLOTS * i - inside) & (LANES - 1), 1))
        a = jnp.where(lane < 40, g[0], jnp.where(lane < 80, g[1], jnp.where(lane < 120, g[2], g[3])))
        b = jnp.where(lane < 32, g[3], jnp.where(lane < 72, g[4], jnp.where(lane < 112, g[5], g[6])))
        c = jnp.where(lane < 24, g[6], g[7])
        packed = jnp.where(low, c[: samples // 2], pltpu.roll(c[samples // 2 :], 64, 1))
        out_ref[o, 0:16, :] = a.astype(BF16)
        out_ref[o, 16:32, :] = b.astype(BF16)
        out_ref[o, 32:40, :] = packed.astype(BF16)
        return carry

    lax.fori_loop(0, out_ref.shape[0], owner, 0, unroll=8)


def gather_blocks(gene_block, counts, owners):
    return pl.pallas_call(
        gather_kernel,
        out_shape=jax.ShapeDtypeStruct((owners, 40, LANES), BF16),
        in_specs=[HBM, HBM],
        out_specs=VMEM,
        scratch_shapes=[
            pltpu.SMEM(gene_block.shape, jnp.int32),
            pltpu.VMEM((counts.shape[0], counts.shape[1] + LANES), BF16),
            pltpu.SemaphoreType.DMA((2,)),
        ],
        compiler_params=pltpu.CompilerParams(vmem_limit_bytes=ALL_VMEM),
        cost_estimate=cost(10_000_000, 1),
        name="gather_blocks",
    )(gene_block, counts)


def tables_kernel(expr_ref, sizes_ref, valid_ref, same_ref, live_ref, kept_ref):
    kept_ref[...] = expr_ref[...]
    me = lax.axis_index("genes")
    first = me * GENE_DEV
    start = pl.multiple_of(first // LANES * LANES, LANES)
    back = (LANES - first % LANES) & (LANES - 1)
    sizes = pltpu.roll(sizes_ref[:, pl.ds(start, LANES)].astype(F32), back, 1)
    valid = pltpu.roll(valid_ref[:, pl.ds(start, LANES)].astype(F32), back, 1)
    ends, running = [], jnp.zeros((1, LANES), F32)
    for c in range(CLUST):
        running = running + sizes[c : c + 1, :]
        ends.append(running)
    ends = jnp.concatenate(ends, axis=0)

    x = lax.broadcasted_iota(jnp.int32, (LANES, WIDE), 1)
    i = lax.broadcasted_iota(jnp.int32, (LANES, WIDE), 0)
    spread = jnp.where((x >= SLOTS * i) & (x < SLOTS * i + SLOTS) & (i < GENE_DEV), 1.0, 0.0)
    spread = spread.astype(BF16)

    def slots_of(rows):
        x = lax.broadcasted_iota(jnp.int32, (rows, WIDE), 1)
        base = jnp.zeros((rows, WIDE), jnp.int32)
        for gene in range(1, GENE_DEV + 1):
            base = jnp.where(x >= SLOTS * gene, SLOTS * gene, base)
        return base, x - base

    ends_at = jnp.dot(ends.astype(BF16), spread, preferred_element_type=F32)
    base, slot = slots_of(CLUST)
    slot = slot.astype(F32)
    low = jnp.max(jnp.where(ends_at <= slot, ends_at, 0.0), axis=0, keepdims=True)
    high = jnp.min(jnp.where(ends_at > slot, ends_at, float(SLOTS)), axis=0, keepdims=True)
    base = base[0:1, :].astype(F32)
    valid_at = jnp.dot(valid.astype(BF16), spread, preferred_element_type=F32)
    _, slot40 = slots_of(SLOTS)
    row40 = lax.broadcasted_iota(jnp.int32, (SLOTS, WIDE), 0)
    live = jnp.sum(jnp.where(slot40 == row40, valid_at, 0.0), axis=0, keepdims=True)

    k = lax.broadcasted_iota(jnp.int32, (WIDE, WIDE), 0).astype(F32)
    inside = (k >= base + low) & (k < base + high)
    same_ref[...] = jnp.where(inside & (k < float(SLOTS * GENE_DEV)), 1.0, 0.0).astype(BF16)
    live_ref[...] = jnp.broadcast_to(live, (8, WIDE))


def make_tables(expression, sizes, valid):
    return pl.pallas_call(
        tables_kernel,
        out_shape=(
            jax.ShapeDtypeStruct((WIDE, WIDE), BF16),
            jax.ShapeDtypeStruct((8, WIDE), F32),
            jax.ShapeDtypeStruct(expression.shape, expression.dtype),
        ),
        in_specs=[VMEM] * 3,
        out_specs=(VMEM,) * 3,
        compiler_params=params(16),
        cost_estimate=cost(10_000_000, 1_000_000),
        name="make_tables",
    )(expression, sizes, valid)


def panel_kernel(recv_ref, same_ref, live_ref, expr_ref, keep_ref, give_ref):
    first_core = lax.axis_index("samples") == 0
    live = live_ref[0:1, :]
    same = same_ref[...]
    per = LANES // 16
    for t in range(recv_ref.shape[0] // per):
        piece = recv_ref[t * per : (t + 1) * per].astype(F32)
        a = piece[:, 0:16, :].reshape(LANES, LANES)
        b = piece[:, 16:32, :].reshape(LANES, LANES)
        c = piece[:, 32:40, :]
        swapped = pltpu.roll(c, 64, 2)
        c = jnp.concatenate([c, swapped], axis=1).reshape(LANES, LANES)
        counts = jnp.concatenate([a, b, c], axis=1) * live
        total = jnp.dot(counts.astype(BF16), same, preferred_element_type=F32)
        ratio = counts / jnp.maximum(total, 1.0)
        lanes = slice(t * LANES, (t + 1) * LANES)
        turned = jnp.transpose(ratio)
        low_half, high_half = turned[0:RATIOS], turned[RATIOS : 2 * RATIOS]
        keep_ref[0:RATIOS, lanes] = jnp.where(first_core, low_half, high_half).astype(BF16)
        give_ref[0:RATIOS, lanes] = jnp.where(first_core, high_half, low_half).astype(BF16)
    expr = expr_ref[...].astype(F32)
    row = lax.broadcasted_iota(jnp.int32, expr.shape, 0)
    low_half = jnp.where(row < GROUP, expr, 1.0)
    high_half = jnp.where(row < GROUP, pltpu.roll(expr, GROUP, 0), 1.0)
    keep_ref[RATIOS:ROWS, :] = jnp.where(first_core, low_half, high_half).astype(BF16)
    give_ref[RATIOS:ROWS, :] = jnp.where(first_core, high_half, low_half).astype(BF16)


def make_panel(recv, tables):
    half = jax.ShapeDtypeStruct((ROWS, tables[2].shape[1]), BF16)
    return pl.pallas_call(
        panel_kernel,
        out_shape=(half, half),
        in_specs=[VMEM] * 4,
        out_specs=(VMEM, VMEM),
        compiler_params=params(16),
        cost_estimate=cost(400_000_000, 2_000_000),
        name="make_panel",
    )(recv, *tables)


NT = (((1,), (1,)), ((), ()))


def row_sums(panels):
    rows = panels[0].shape[0]
    one, two = jnp.zeros((rows, LANES), F32), jnp.zeros((rows, LANES), F32)
    for panel in panels:
        for t in range(panel.shape[1] // LANES):
            p = panel[:, t * LANES : (t + 1) * LANES].astype(F32)
            one, two = one + p, two + p * p
    return jnp.sum(one, axis=1, keepdims=True), jnp.sum(two, axis=1, keepdims=True)


BLOCK = 256


def dose_kernel(count, dose_hbm, other_hbm, dose_ref, other_ref, stats_ref, sems):
    blocks = dose_ref.shape[0] // BLOCK
    copies = [
        [
            pltpu.make_async_copy(
                source.at[pl.ds(i * BLOCK, BLOCK)], to.at[pl.ds(i * BLOCK, BLOCK)], sems.at[side, i]
            )
            for side, (source, to) in enumerate(((dose_hbm, dose_ref), (other_hbm, other_ref)))
        ]
        for i in range(blocks)
    ]
    for pair in copies:
        for copy in pair:
            copy.start()
    row = lax.broadcasted_iota(jnp.int32, (8, BLOCK), 0)
    for i, pair in enumerate(copies):
        one, two = jnp.zeros((BLOCK, LANES), F32), jnp.zeros((BLOCK, LANES), F32)
        for copy, ref in zip(pair, (dose_ref, other_ref)):
            copy.wait()
            for t in range(ref.shape[1] // LANES):
                d = ref[i * BLOCK : (i + 1) * BLOCK, t * LANES : (t + 1) * LANES].astype(F32)
                one, two = one + d, two + d * d
        sx = jnp.sum(jnp.transpose(one), axis=0, keepdims=True)
        sxx = jnp.sum(jnp.transpose(two), axis=0, keepdims=True)
        scale = lax.rsqrt(jnp.maximum(sxx - sx * sx / count, 1.0))
        stats_ref[:, i * BLOCK : (i + 1) * BLOCK] = jnp.where(row == 0, sx, scale)


def dose_stats(dosage, other, count):
    rows = dosage.shape[0]
    same = jax.ShapeDtypeStruct(dosage.shape, dosage.dtype)
    return pl.pallas_call(
        functools.partial(dose_kernel, count),
        out_shape=(same, same, jax.ShapeDtypeStruct((8, rows), F32)),
        in_specs=[HBM, HBM],
        out_specs=(VMEM,) * 3,
        scratch_shapes=[pltpu.SemaphoreType.DMA((2, rows // BLOCK))],
        compiler_params=params(LIM),
        cost_estimate=cost(20_000_000, 16_000_000),
        name="dose_stats",
    )(dosage, other)


def correlations(count, keep_ref, got_ref, stats_ref, doses, put):
    sy, syy = row_sums((keep_ref, got_ref))
    mean = sy / count
    scale = lax.rsqrt(jnp.maximum(syy - sy * mean, 1.0))
    dose_ref, other_ref = doses
    for i in range(W // BLOCK):
        lanes = slice(i * BLOCK, (i + 1) * BLOCK)
        cross = lax.dot_general(keep_ref[...], dose_ref[lanes], NT, preferred_element_type=F32)
        cross = cross + lax.dot_general(
            got_ref[...], other_ref[lanes], NT, preferred_element_type=F32
        )
        put(lanes, (cross - stats_ref[0:1, lanes] * mean) * stats_ref[1:2, lanes] * scale)


def own_product(window_start, keep, got, stats, doses, count):
    side = jax.ShapeDtypeStruct((ROWS, HALF), BF16)

    def kernel(start_ref, keep_ref, got_ref, stats_ref, *refs):
        doses, (mine_ref, theirs_ref, wide) = refs[:2], refs[2:]
        core = lax.axis_index("samples")

        def put(lanes, values):
            wide[:, lanes] = values

        correlations(count, keep_ref, got_ref, stats_ref, doses, put)
        wide[:, W : W + SPILL] = jnp.zeros((ROWS, SPILL), F32)
        for ref, side in ((theirs_ref, 1 - core), (mine_ref, core)):
            last = []
            for j in range(GROUP):
                begin = start_ref[GROUP * core + j] + side * HALF
                window = pl.ds(pl.multiple_of(begin, LANES), HALF)
                rows = slice(SLOTS * j, SLOTS * j + SLOTS)
                ref[rows, :] = wide[rows, window].astype(BF16)
                last.append(wide[RATIOS + j : RATIOS + j + 1, window])
            last = jnp.concatenate(last + last, axis=0)
            ref[RATIOS:ROWS, :] = last.astype(BF16)

    return pl.pallas_call(
        kernel,
        out_shape=(side, side),
        in_specs=[SMEM] + [VMEM] * 5,
        out_specs=(VMEM, VMEM),
        scratch_shapes=[pltpu.VMEM((ROWS, W + SPILL), F32)],
        compiler_params=params(16),
        cost_estimate=cost(1_500_000_000, 12_000_000),
        name="own_product",
    )(window_start, keep, got, stats, *doses)


def spill_first(keep, dose):
    def kernel(keep_ref, dose_ref, out_ref):
        for i in range(SPILL // BLOCK):
            lanes = slice(i * BLOCK, (i + 1) * BLOCK)
            out_ref[:, lanes] = lax.dot_general(
                keep_ref[...], dose_ref[lanes], NT, preferred_element_type=F32
            )
        sy, syy = row_sums((keep_ref,))
        lane = lax.broadcasted_iota(jnp.int32, (ROWS, LANES), 1)
        out_ref[:, SPILL : SPILL + LANES] = jnp.where(lane == 0, sy, syy)

    return pl.pallas_call(
        kernel,
        out_shape=jax.ShapeDtypeStruct((ROWS, SPILL + LANES), F32),
        in_specs=[VMEM] * 2,
        out_specs=VMEM,
        compiler_params=params(16),
        cost_estimate=cost(350_000_000, 3_000_000),
        name="spill_first",
    )(keep, dose)


def spill_product(part, got, stats, other, count):
    def kernel(part_ref, got_ref, stats_ref, other_ref, out_ref):
        sy, syy = row_sums((got_ref,))
        sy = sy + part_ref[:, SPILL : SPILL + 1]
        syy = syy + part_ref[:, SPILL + 1 : SPILL + 2]
        mean = sy / count
        scale = lax.rsqrt(jnp.maximum(syy - sy * mean, 1.0))
        for i in range(SPILL // BLOCK):
            lanes = slice(i * BLOCK, (i + 1) * BLOCK)
            cross = part_ref[:, lanes] + lax.dot_general(
                got_ref[...], other_ref[lanes], NT, preferred_element_type=F32
            )
            value = (cross - stats_ref[0:1, lanes] * mean) * stats_ref[1:2, lanes] * scale
            out_ref[:, lanes] = value.astype(BF16)

    return pl.pallas_call(
        kernel,
        out_shape=jax.ShapeDtypeStruct((ROWS, SPILL), BF16),
        in_specs=[VMEM] * 4,
        out_specs=VMEM,
        compiler_params=params(16),
        cost_estimate=cost(350_000_000, 3_000_000),
        name="spill_product",
    )(part, got, stats, other)


def merge_kernel(start_ref, mine_ref, other_ref, back0, back1, out_hbm, wide, rows48, out_ref, sems):
    core = lax.axis_index("samples")
    back = (back0, back1)
    for c in range(2):
        wide[c, :, SPILL : 2 * SPILL] = back[c][...].astype(F32)
    for own_ref, c in ((mine_ref, core), (other_ref, 1 - core)):
        every = own_ref[...].astype(F32)
        for j in range(GROUP):
            begin = start_ref[GROUP * c + j]
            window = pl.ds(pl.multiple_of(begin, LANES), HALF)
            edge = jnp.where(core == 1, HALF - begin, HALF)
            at = 48 * (GROUP * c + j)
            for rows, to in (
                (slice(SLOTS * j, SLOTS * j + SLOTS), pl.ds(pl.multiple_of(at, 8), SLOTS)),
                (slice(RATIOS + j, RATIOS + j + 1), pl.ds(at + SLOTS, 1)),
            ):
                own = every[rows, :]
                lane = lax.broadcasted_iota(jnp.int32, own.shape, 1)
                value = jnp.where(lane >= edge, wide[c, rows, window], own)
                for t in range(HALF // LANES):
                    rows48[t, to, :] = value[:, t * LANES : (t + 1) * LANES]
    copies = []
    for k, first in enumerate(range(0, SLOTS + 1, PIECE)):
        end = min(first + PIECE, SLOTS + 1)
        for p in range(first, end):
            row = SLOTS if p == 0 else p - 1
            for t in range(HALF // LANES):
                genes = rows48[t, pl.ds(row, GENE_DEV, stride=48), :]
                out_ref[p, :, t * LANES : (t + 1) * LANES] = genes.astype(BF16)
        part = pl.ds(first, end - first)
        copies.append(pltpu.make_async_copy(out_ref.at[part], out_hbm.at[part], sems.at[k]))
        copies[-1].start()
    for copy in copies:
        copy.wait()


PIECE = 11


def merge(window_start, mine, other, back):
    return pl.pallas_call(
        merge_kernel,
        out_shape=jax.ShapeDtypeStruct((SLOTS + 1, GENE_DEV, HALF), BF16),
        in_specs=[SMEM] + [VMEM] * 4,
        out_specs=HBM,
        scratch_shapes=[
            pltpu.VMEM((2, ROWS, 2 * SPILL), F32),
            pltpu.VMEM((HALF // LANES, 48 * GENE_DEV, LANES), F32),
            pltpu.VMEM((SLOTS + 1, GENE_DEV, HALF), BF16),
            pltpu.SemaphoreType.DMA((pl.cdiv(SLOTS + 1, PIECE),)),
        ],
        compiler_params=params(24),
        cost_estimate=cost(2_000_000, 3_500_000),
        name="merge_windows",
    )(window_start, mine, other, *back)


def shards(dosage, expression, intron_counts, cluster_sizes, valid_mask, gene_block, window_start):
    owners = lax.axis_size("genes")
    cores = lax.axis_size("samples")
    count = float(dosage.shape[1] * cores)
    onward = [(i, i + 1) for i in range(owners - 1)]
    swap = [(i, cores - 1 - i) for i in range(cores)]
    last = cores - 1
    home = [
        [((i + 1) * cores + c, i * cores + last) for i in range(owners - 1)] for c in range(cores)
    ]
    sizes, valid = cluster_sizes.T, valid_mask.T

    def exchanged(x):
        return lax.ppermute(x, "samples", swap)

    other_dose = exchanged(dosage)
    blocks = gather_blocks(gene_block, intron_counts, owners)
    recv = lax.all_to_all(blocks, "genes", 0, 0, tiled=True)
    tables = make_tables(expression, sizes, valid)
    *doses, stats = dose_stats(dosage, other_dose, count)

    keep, give = make_panel(recv, tables)
    got = exchanged(give)
    passed_keep = lax.ppermute(keep, "genes", onward)
    passed_got = lax.ppermute(got, "genes", onward)
    mine, theirs = own_product(window_start, keep, got, stats, doses, count)
    other = exchanged(theirs)

    part = spill_first(passed_keep, doses[0])
    piece = spill_product(part, passed_got, stats, doses[1], count)
    back = []
    for c in range(cores):
        back.append(lax.ppermute(piece, ("genes", "samples"), home[c]))
    out = merge(window_start, mine, other, back)
    return jnp.transpose(out, (1, 0, 2))


def solution(mesh):
    in_specs = (
        P(("parts", "genes"), "samples"),
        P(("parts", "genes"), "samples"),
        P(("parts", "samples", "genes"), None),
        P("parts", None),
        P("parts", None),
        P("parts"),
        P(("parts", "genes")),
    )
    out_specs = P(("parts", "genes"), None, "samples")
    return jax.shard_map(shards, mesh=mesh, in_specs=in_specs, out_specs=out_specs, check_vma=False)
```
